32 devices in a mesh: shard: 2 (over core), ctx: 4 (over y, x), tensor: 4 (over z).
Axes of the slice: x: 2, y: 2, z: 4, core: 2. Of those that a mesh axis runs over, the one named last changes fastest.
Arguments:
- block_input: bfloat16 [4, 2048, 1536], P('shard', 'ctx', 'tensor'), may hold values from -6 to 6
- output_cotangent: bfloat16 [4, 2048, 1536], P('shard', 'ctx', 'tensor'), may hold values from -6 to 6
- norm_gain: bfloat16 [1536], P(('shard', 'ctx')), may hold values from 0.099609375 to 1.8984375
- gate_value_weight: bfloat16 [1536, 2, 3072], P(('shard', 'ctx'), None, 'tensor'), may hold values from -0.15625 to 0.15625
- matrix_weight: bfloat16 [1536, 256], P(('shard', 'ctx')), may hold values from -0.15625 to 0.15625
- step_weight: bfloat16 [1536, 48], P(('shard', 'ctx'), 'tensor'), may hold values from -0.15625 to 0.15625
- out_weight: bfloat16 [1536, 3072], P(('shard', 'ctx'), 'tensor'), may hold values from -0.109375 to 0.109375
- value_kernel: float32 [4, 3072], P(None, 'tensor'), may hold values from -3 to 3
- value_bias: float32 [3072], P('tensor'), may hold values from -3 to 3
- matrix_kernel: float32 [4, 256], replicated, may hold values from -3 to 3
- matrix_bias: float32 [256], replicated, may hold values from -3 to 3
- step_bias: float32 [48], P('tensor'), may hold values from -7 to -3
- decay_log: float32 [48], P('tensor'), may hold values from -4 to 1
- skip_gain: float32 [48], P('tensor'), may hold values from 0.5 to 1.5
- inner_gain: float32 [3072], P('tensor'), may hold values from 0.1 to 1.9
Outputs:
- block_output: bfloat16 [4, 2048, 1536], P('shard', 'ctx', 'tensor')
- input_grad: float32 [4, 2048, 1536], P('shard', 'ctx', 'tensor')
- norm_gain_grad: float32 [1536], P(('shard', 'ctx'))
- gate_value_grad: float32 [1536, 2, 3072], P(('shard', 'ctx'), None, 'tensor')
- matrix_weight_grad: float32 [1536, 256], P(('shard', 'ctx'))
- step_weight_grad: float32 [1536, 48], P(('shard', 'ctx'), 'tensor')
- out_weight_grad: float32 [1536, 3072], P(('shard', 'ctx'), 'tensor')
- value_kernel_grad: float32 [4, 3072], P(None, 'tensor')
- value_bias_grad: float32 [3072], P('tensor')
- matrix_kernel_grad: float32 [4, 256], replicated
- matrix_bias_grad: float32 [256], replicated
- step_bias_grad: float32 [48], P('tensor')
- decay_log_grad: float32 [48], P('tensor')
- skip_gain_grad: float32 [48], P('tensor')
- inner_gain_grad: float32 [3072], P('tensor')
The draws below stay inside these ranges and needn't reach their ends.
All inputs are finite; a program needn't handle non-finite values.
Results may differ from the reference program's by a relative error of at most 0.012.
Values may be sent and summed in bfloat16 or wider, within the bound.
A program may use at most 192 MiB of HBM per device.

```python
import jax
import jax.numpy as jnp
from jax import lax

D = 1536
HEADS = 48
HEAD_DIM = 64
STATE = 128
KERNEL = 4
BLOCK = 256
INNER = 3072
SEQS = 4
LENGTH = 2048


def block_levels(stream_key, extent, shards, low, top_value):
    def one(dim, blocks):
        heights = jax.random.uniform(jax.random.fold_in(jax.random.fold_in(stream_key, 6), dim), (blocks,), jnp.float32, low / len(shards), top_value / len(shards))
        return jnp.repeat(jnp.exp(heights), extent[dim] // blocks).reshape((-1,) + (1,) * (len(extent) - dim - 1))

    level = one(*shards[0])
    for cut in shards[1:]:
        level = level * one(*cut)
    return level


def noise(key, shape, scale, most, split=(), dtype=jnp.bfloat16):
    result = scale * jax.random.normal(key, shape, jnp.float32)
    if split:
        result = result * block_levels(key, shape, split, -0.22, 0.18)
    return jnp.clip(result, -most, most).astype(dtype)


def setup_inputs(seed: int = 0) -> dict:
    seeds = jax.random.split(jax.random.key(seed), 16)
    block_input = noise(seeds[0], (SEQS, LENGTH, D), 1.0, 6.0, ((0, 2), (1, 4), (2, 4)))
    output_cotangent = noise(seeds[1], (SEQS, LENGTH, D), 1.0, 6.0, ((0, 2), (1, 4), (2, 4)))
    norm_gain = jnp.clip(1.0 + 0.18 * jax.random.normal(seeds[2], (D,), jnp.float32), 0.099609375, 1.8984375).astype(jnp.bfloat16)
    gate_value_weight = noise(seeds[3], (D, 2, INNER), D ** -0.5, 0.15625, ((0, 8), (2, 4)))
    matrix_weight = noise(seeds[4], (D, 2 * STATE), D ** -0.5, 0.15625, ((0, 8),))
    step_weight = noise(seeds[5], (D, HEADS), D ** -0.5, 0.15625, ((0, 8), (1, 4)))
    out_weight = noise(seeds[6], (D, INNER), INNER ** -0.5, 0.109375, ((0, 8), (1, 4)))
    value_kernel = noise(seeds[7], (KERNEL, INNER), 0.5, 3.0, ((1, 4),), jnp.float32)
    value_bias = noise(seeds[8], (INNER,), 0.5, 3.0, ((0, 4),), jnp.float32)
    matrix_kernel = noise(seeds[9], (KERNEL, 2 * STATE), 0.5, 3.0, (), jnp.float32)
    matrix_bias = noise(seeds[10], (2 * STATE,), 0.5, 3.0, (), jnp.float32)
    step_bias = jnp.clip(-7.0 + 4.0 * jax.random.uniform(seeds[11], (HEADS,), jnp.float32) ** block_levels(seeds[11], (HEADS,), ((0, 4),), -0.2, 0.2), -7.0, -3.0)
    decay_log = jnp.clip(-4.0 + 5.0 * jax.random.uniform(seeds[12], (HEADS,), jnp.float32) ** block_levels(seeds[12], (HEADS,), ((0, 4),), -0.2, 0.2), -4.0, 1.0)
    skip_gain = jnp.clip(0.5 + 1.0 * jax.random.uniform(seeds[13], (HEADS,), jnp.float32) ** block_levels(seeds[13], (HEADS,), ((0, 4),), -0.2, 0.2), 0.5, 1.5)
    inner_gain = jnp.clip(1.0 + 0.18 * jax.random.normal(seeds[14], (INNER,), jnp.float32), 0.1, 1.9)
    return dict(block_input=block_input, output_cotangent=output_cotangent, norm_gain=norm_gain, gate_value_weight=gate_value_weight, matrix_weight=matrix_weight, step_weight=step_weight, out_weight=out_weight, value_kernel=value_kernel, value_bias=value_bias, matrix_kernel=matrix_kernel, matrix_bias=matrix_bias, step_bias=step_bias, decay_log=decay_log, skip_gain=skip_gain, inner_gain=inner_gain)


HIGHEST = lax.Precision.HIGHEST
EPSILON = 1e-05

def rounded(value):
    return lax.optimization_barrier(value.astype(jnp.bfloat16)).astype(jnp.float32)

def silu_slope(value):
    sigma = jax.nn.sigmoid(value)
    return sigma * (1.0 + value * (1.0 - sigma))

def dot_rows(left, right):
    return lax.dot_general(left, right, (((1,), (1,)), ((), ())), preferred_element_type=jnp.float32)

def dot_tokens(left, right):
    return lax.dot_general(left, right, (((0,), (0,)), ((), ())), preferred_element_type=jnp.float32)

def causal_conv(signal, before, kernel, bias):
    kernel_width = kernel.shape[0]
    seq_rows = signal.shape[-2]
    padded = jnp.concatenate([before, signal], axis=-2)
    total = jnp.zeros_like(signal) + bias
    for offset in range(kernel_width):
        total = total + kernel[offset] * padded[..., offset:offset + seq_rows, :]
    return total

def conv_transpose(grad, after, kernel):
    kernel_width = kernel.shape[0]
    seq_rows = grad.shape[-2]
    padded = jnp.concatenate([grad, after], axis=-2)
    total = jnp.zeros_like(grad)
    for offset in range(kernel_width):
        first = kernel_width - 1 - offset
        total = total + kernel[offset] * padded[..., first:first + seq_rows, :]
    return total

def kernel_grad(grad, signal, before):
    kernel_width = before.shape[-2] + 1
    seq_rows = grad.shape[-2]
    padded = jnp.concatenate([before, signal], axis=-2)
    summed_axes = tuple(range(grad.ndim - 1))
    return jnp.stack([lax.optimization_barrier(jnp.sum(grad * padded[..., offset:offset + seq_rows, :], axis=summed_axes)) for offset in range(kernel_width)])

def decay_matrix(cum_decay):
    by_head = cum_decay.T
    spread = by_head[:, :, None] - by_head[:, None, :]
    token_count = cum_decay.shape[0]
    causal = (jnp.arange(token_count)[:, None] >= jnp.arange(token_count)[None, :])[None]
    return jnp.where(causal, jnp.exp(jnp.where(causal, spread, 0.0)), 0.0)

def block_forward(values, b_matrix, c_matrix, log_decay, step_size, start):
    cum_decay = jnp.cumsum(log_decay, axis=0)
    weights = decay_matrix(cum_decay) * jnp.dot(c_matrix, b_matrix.T, precision=HIGHEST)[None]
    scaled = values * step_size[:, :, None]
    inside = jnp.einsum('hts,shp->thp', weights, scaled, precision=HIGHEST)
    carried = jnp.exp(cum_decay)[:, :, None] * jnp.einsum('tn,hnp->thp', c_matrix, start, precision=HIGHEST)
    to_end = jnp.exp(cum_decay[-1][None, :] - cum_decay)
    final_state = jnp.exp(cum_decay[-1])[:, None, None] * start + jnp.einsum('sn,shp->hnp', b_matrix, scaled * to_end[:, :, None], precision=HIGHEST)
    return (inside + carried, final_state)

def block_backward(values, b_matrix, c_matrix, log_decay, step_size, start, ssd_part, grad_part, incoming):
    cum_decay = jnp.cumsum(log_decay, axis=0)
    decays = decay_matrix(cum_decay)
    weights = decays * jnp.dot(c_matrix, b_matrix.T, precision=HIGHEST)[None]
    to_end = jnp.exp(cum_decay[-1][None, :] - cum_decay)
    from_start = jnp.exp(cum_decay)
    b_dot = jnp.einsum('hts,thp->shp', weights, grad_part, precision=HIGHEST) + to_end[:, :, None] * jnp.einsum('sn,hnp->shp', b_matrix, incoming, precision=HIGHEST)
    pair_dots = jnp.einsum('thp,shp->hts', grad_part, values, precision=HIGHEST)
    mixing = jnp.einsum('hts,sh->ts', decays * pair_dots, step_size, precision=HIGHEST)
    grad_b = jnp.dot(mixing.T, c_matrix, precision=HIGHEST) + jnp.einsum('shp,hnp->sn', values * (step_size * to_end)[:, :, None], incoming, precision=HIGHEST)
    weighted_grad = grad_part * from_start[:, :, None]
    grad_c = jnp.dot(mixing, b_matrix, precision=HIGHEST) + jnp.einsum('thp,hnp->tn', weighted_grad, start, precision=HIGHEST)
    earlier = jnp.exp(cum_decay[-1])[:, None, None] * incoming + jnp.einsum('tn,thp->hnp', c_matrix, weighted_grad, precision=HIGHEST)
    value_dot = lax.optimization_barrier(jnp.sum(values * b_dot, axis=2))
    cum_grad = lax.optimization_barrier(jnp.sum(grad_part * ssd_part, axis=2)) - step_size * value_dot
    return (earlier, (b_dot, grad_b, grad_c, value_dot, cum_grad))

def run_forward(values, b_matrix, c_matrix, log_decay, step_size, start):
    seq_rows = values.shape[0]
    block_count = seq_rows // BLOCK

    def blocks(array):
        return array.reshape((block_count, BLOCK) + array.shape[1:])

    def advance(current, pieces):
        output, final_state = block_forward(*pieces, current)
        return (final_state, (output, current))
    unused, (outputs, starts) = lax.scan(advance, start, (blocks(values), blocks(b_matrix), blocks(c_matrix), blocks(log_decay), blocks(step_size)))
    return (outputs.reshape(values.shape), starts)

def run_backward(values, b_matrix, c_matrix, log_decay, step_size, starts, ssd_out, grad_mixed, incoming):
    seq_rows = values.shape[0]
    block_count = seq_rows // BLOCK

    def blocks(array):
        return array.reshape((block_count, BLOCK) + array.shape[1:])

    def retreat(current, pieces):
        return block_backward(*pieces, current)
    unused, results = lax.scan(retreat, incoming, (blocks(values), blocks(b_matrix), blocks(c_matrix), blocks(log_decay), blocks(step_size), starts, blocks(ssd_out), blocks(grad_mixed)), reverse=True)
    return tuple((item.reshape((seq_rows,) + item.shape[2:]) for item in results))

def one_sequence(seq_input, seq_cot, params):
    norm_gain, gate_value_weight, matrix_weight, step_weight, out_weight, value_kernel, value_bias, matrix_kernel, matrix_bias, step_bias, decay_log, skip_gain, inner_gain = params
    seq_rows = seq_input.shape[0]
    inputs = seq_input.astype(jnp.float32)
    input_scale = lax.rsqrt(lax.optimization_barrier(jnp.mean(inputs * inputs, axis=1, keepdims=True)) + EPSILON)
    normalized = inputs * input_scale
    normed = (normalized * norm_gain.astype(jnp.float32)[None, :]).astype(jnp.bfloat16)
    flat_gate_value = gate_value_weight.reshape(D, 2 * INNER)
    gate_value = rounded(jnp.dot(normed, flat_gate_value, preferred_element_type=jnp.float32))
    gate = gate_value[:, :INNER]
    values_in = gate_value[:, INNER:]
    matrix_in = rounded(jnp.dot(normed, matrix_weight, preferred_element_type=jnp.float32))
    step_raw = jnp.dot(normed, step_weight, preferred_element_type=jnp.float32)
    edge_values = jnp.zeros((KERNEL - 1, INNER), jnp.float32)
    edge_matrix = jnp.zeros((KERNEL - 1, 2 * STATE), jnp.float32)
    value_conv = causal_conv(values_in, edge_values, value_kernel, value_bias)
    values = jax.nn.silu(value_conv)
    matrix_conv = causal_conv(matrix_in, edge_matrix, matrix_kernel, matrix_bias)
    matrices = jax.nn.silu(matrix_conv)
    b_matrix = matrices[:, :STATE]
    c_matrix = matrices[:, STATE:]
    step_size = jax.nn.softplus(step_raw + step_bias[None, :])
    rate = -jnp.exp(decay_log)
    log_decay = step_size * rate[None, :]
    value_heads = values.reshape(seq_rows, HEADS, HEAD_DIM)
    zero_state = jnp.zeros((HEADS, STATE, HEAD_DIM), jnp.float32)
    ssd_out, starts = run_forward(value_heads, b_matrix, c_matrix, log_decay, step_size, zero_state)
    mixed = (ssd_out + skip_gain[None, :, None] * value_heads).reshape(seq_rows, INNER)
    gate_act = jax.nn.silu(gate)
    gated = mixed * gate_act
    inner_scale = lax.rsqrt(lax.optimization_barrier(jnp.mean(gated * gated, axis=1, keepdims=True)) + EPSILON)
    normed_inner = (gated * inner_scale * inner_gain[None, :]).astype(jnp.bfloat16)
    output = (inputs + dot_rows(normed_inner, out_weight)).astype(jnp.bfloat16)
    grad_inner = jnp.dot(seq_cot, out_weight, preferred_element_type=jnp.float32)
    out_grad = dot_tokens(seq_cot, normed_inner)
    inner_gain_grad = lax.optimization_barrier(jnp.sum(grad_inner * gated * inner_scale, axis=0))
    scaled_grad = grad_inner * inner_gain[None, :]
    row_dot = lax.optimization_barrier(jnp.mean(scaled_grad * gated, axis=1, keepdims=True))
    grad_gated = inner_scale * scaled_grad - gated * inner_scale ** 3 * row_dot
    grad_mixed = (grad_gated * gate_act).reshape(seq_rows, HEADS, HEAD_DIM)
    grad_gate = grad_gated * mixed * silu_slope(gate)
    skip_grad = lax.optimization_barrier(jnp.sum(grad_mixed * value_heads, axis=(0, 2)))
    b_dot, grad_b, grad_c, value_dot, cum_grad = run_backward(value_heads, b_matrix, c_matrix, log_decay, step_size, starts, ssd_out, grad_mixed, zero_state)
    grad_log = jnp.flip(jnp.cumsum(jnp.flip(cum_grad, 0), axis=0), 0)
    grad_values = (step_size[:, :, None] * b_dot + skip_gain[None, :, None] * grad_mixed).reshape(seq_rows, INNER)
    grad_step = value_dot + grad_log * rate[None, :]
    decay_grad = rate * lax.optimization_barrier(jnp.sum(grad_log * step_size, axis=0))
    grad_raw = grad_step * jax.nn.sigmoid(step_raw + step_bias[None, :])
    step_bias_grad = lax.optimization_barrier(jnp.sum(grad_raw, axis=0))
    grad_value_conv = grad_values * silu_slope(value_conv)
    grad_matrix_conv = jnp.concatenate([grad_b, grad_c], axis=1) * silu_slope(matrix_conv)
    grad_values_in = conv_transpose(grad_value_conv, edge_values, value_kernel)
    grad_matrix_in = conv_transpose(grad_matrix_conv, edge_matrix, matrix_kernel)
    value_kernel_grad = kernel_grad(grad_value_conv, values_in, edge_values)
    value_bias_grad = lax.optimization_barrier(jnp.sum(grad_value_conv, axis=0))
    matrix_kernel_grad = kernel_grad(grad_matrix_conv, matrix_in, edge_matrix)
    matrix_bias_grad = lax.optimization_barrier(jnp.sum(grad_matrix_conv, axis=0))
    grad_gate_value = jnp.concatenate([grad_gate, grad_values_in], axis=1).astype(jnp.bfloat16)
    grad_matrix_low = grad_matrix_in.astype(jnp.bfloat16)
    grad_raw_low = grad_raw.astype(jnp.bfloat16)
    grad_normed = dot_rows(grad_gate_value, flat_gate_value) + dot_rows(grad_matrix_low, matrix_weight) + dot_rows(grad_raw_low, step_weight)
    gate_value_grad = dot_tokens(normed, grad_gate_value).reshape(D, 2, INNER)
    matrix_grad = dot_tokens(normed, grad_matrix_low)
    step_grad = dot_tokens(normed, grad_raw_low)
    norm_grad = lax.optimization_barrier(jnp.sum(grad_normed * normalized, axis=0))
    grad_hat = grad_normed * norm_gain.astype(jnp.float32)[None, :]
    input_grad = input_scale * (grad_hat - normalized * lax.optimization_barrier(jnp.mean(grad_hat * normalized, axis=1, keepdims=True))) + seq_cot.astype(jnp.float32)
    grads = (norm_grad, gate_value_grad, matrix_grad, step_grad, out_grad, value_kernel_grad, value_bias_grad, matrix_kernel_grad, matrix_bias_grad, step_bias_grad, decay_grad, skip_grad, inner_gain_grad)
    return ((output, input_grad), grads)

def reference(block_input, output_cotangent, norm_gain, gate_value_weight, matrix_weight, step_weight, out_weight, value_kernel, value_bias, matrix_kernel, matrix_bias, step_bias, decay_log, skip_gain, inner_gain):
    params = (norm_gain, gate_value_weight, matrix_weight, step_weight, out_weight, value_kernel, value_bias, matrix_kernel, matrix_bias, step_bias, decay_log, skip_gain, inner_gain)
    zero_grads = tuple((jnp.zeros(param.shape, jnp.float32) for param in params))

    def advance(totals, pieces):
        outputs, grads = one_sequence(pieces[0], pieces[1], params)
        return (tuple((total_part + grad_part for total_part, grad_part in zip(totals, grads))), outputs)
    totals, (outputs, input_grads) = lax.scan(advance, zero_grads, (block_input, output_cotangent))
    return (outputs, input_grads) + totals
```

```python
import functools

import jax
import jax.numpy as jnp
from jax import lax
from jax.experimental import pallas as pl
from jax.experimental.pallas import tpu as pltpu
from jax.sharding import PartitionSpec as P

EPSILON = 1e-05
HALO = 16
CHUNK = 128
LANES = 128
HIGHEST = lax.Precision.HIGHEST
MESH = pl.DeviceIdType.MESH
F32 = jnp.float32
BF16 = jnp.bfloat16
VMEM_ALL = 64000 * 1024
FINE_A = True
FINE_B = True
FINE_C = True
FINE_S = True


def dot_nn(left, right, precision=None):
    return lax.dot_general(
        left, right, (((1,), (0,)), ((), ())), precision=precision, preferred_element_type=F32
    )


def dot_nt(left, right, precision=None):
    return lax.dot_general(
        left, right, (((1,), (1,)), ((), ())), precision=precision, preferred_element_type=F32
    )


def dot_tokens(left, right):
    axes = tuple(range(left.ndim - 1))
    return lax.dot_general(left, right, ((axes, axes), ((), ())), preferred_element_type=F32)


def split(value):
    high = value.astype(BF16)
    return high, (value - high.astype(F32)).astype(BF16)


def fine(dot, left, right):
    (a, b), (c, d) = split(left), split(right)
    return dot(a, c) + (dot(a, d) + dot(b, c))


def vmem_spec():
    return pl.BlockSpec(memory_space=pltpu.VMEM)


def any_spec():
    return pl.BlockSpec(memory_space=pl.ANY)


def sizes():
    return lax.axis_size("shard"), lax.axis_size("ctx"), lax.axis_size("tensor")


def places():
    return lax.axis_index("shard"), lax.axis_index("ctx"), lax.axis_index("tensor")


def remote(src, dst, send_sem, recv_sem, **device):
    return pltpu.make_async_remote_copy(
        src_ref=src,
        dst_ref=dst,
        send_sem=send_sem,
        recv_sem=recv_sem,
        device_id=device,
        device_id_type=MESH,
    )


def greet(peers, count):
    barrier = pltpu.get_barrier_semaphore()
    for condition, device in peers:
        if condition is None:
            pl.semaphore_signal(barrier, inc=1, device_id=device, device_id_type=MESH)
        else:

            @pl.when(condition)
            def _():
                pl.semaphore_signal(barrier, inc=1, device_id=device, device_id_type=MESH)

    pl.semaphore_wait(barrier, count)


def gather_kernel(
    dims, x_ref, gv_ref, ow_ref, sw_ref, X, GV, OW, SW, hv, lsem, hs, hr, zs, zr, cs, cr, ss, sr
):
    ns, nc, nz = dims
    s, c, z = places()
    seqs, length, quarter = x_ref.shape
    half = length // 2
    parts = [(q, h * half) for q in range(seqs) for h in range(2)]
    count = len(parts)

    peers = [(z > 0, {"tensor": z - 1}), (z < nz - 1, {"tensor": z + 1})]
    peers += [(None, {"ctx": lax.rem(c + k, nc)}) for k in range(1, nc)]
    peers += [(None, {"shard": lax.rem(s + j, ns)}) for j in range(1, ns)]
    greet(
        peers,
        jnp.where(z > 0, 1, 0) + jnp.where(z < nz - 1, 1, 0) + (nc - 1) + (ns - 1),
    )

    def columns(owner):
        return pl.ds(pl.multiple_of(owner * quarter, quarter), quarter)

    def region(i, owner):
        if i == count:
            return X.at[:, pl.ds(0, HALO), columns(owner)]
        q, r0 = parts[i]
        return X.at[q, pl.ds(HALO + r0, half), columns(owner)]

    def own(i):
        if i == count:
            return hv
        q, r0 = parts[i]
        return x_ref.at[q, pl.ds(r0, half), :]

    def up(d, i):
        src = own(i) if d == 0 else region(i, z - d)
        return remote(src, region(i, z - d), zs.at[0, d, i], zr.at[0, d, i], tensor=z + 1)

    def down(d, i):
        src = own(i) if d == 0 else region(i, z + d)
        return remote(src, region(i, z + d), zs.at[1, d, i], zr.at[1, d, i], tensor=z - 1)

    def got_up(d, i):
        here = region(i, z - d)
        return remote(here, here, zs.at[0, d - 1, i], zr.at[0, d - 1, i], tensor=z - 1)

    def got_down(d, i):
        here = region(i, z + d)
        return remote(here, here, zs.at[1, d - 1, i], zr.at[1, d - 1, i], tensor=z + 1)

    halo_send = remote(
        x_ref.at[:, pl.ds(length - HALO, HALO), :], hv, hs, hr, ctx=lax.rem(c + 1, nc)
    )

    @pl.when(c < nc - 1)
    def _():
        halo_send.start()

    for i in range(count):

        @pl.when(z < nz - 1)
        def _():
            up(0, i).start()

        @pl.when(z > 0)
        def _():
            down(0, i).start()

    arrays = [(gv_ref, GV), (ow_ref, OW), (sw_ref, SW)]

    def rows(array, shard, ctx):
        block = array[0].shape[0]
        return array[1].at[pl.ds(pl.multiple_of((shard * nc + ctx) * block, block), block), :]

    def to_ctx(k, a):
        array = arrays[a]
        return remote(
            array[0], rows(array, s, c), cs.at[k - 1, a], cr.at[k - 1, a], ctx=lax.rem(c + k, nc)
        )

    def from_ctx(k, a):
        here = rows(arrays[a], s, lax.rem(c + nc - k, nc))
        return remote(
            here, here, cs.at[k - 1, a], cr.at[k - 1, a], ctx=lax.rem(c + nc - k, nc)
        )

    def to_shard(k, j, a):
        array = arrays[a]
        there = rows(array, s, lax.rem(c + nc - k, nc))
        src = array[0] if k == 0 else there
        return remote(
            src, there, ss.at[k, j - 1, a], sr.at[k, j - 1, a], shard=lax.rem(s + j, ns)
        )

    def from_shard(k, j, a):
        owner = lax.rem(s + ns - j, ns)
        here = rows(arrays[a], owner, lax.rem(c + nc - k, nc))
        return remote(here, here, ss.at[k, j - 1, a], sr.at[k, j - 1, a], shard=owner)

    for a in range(3):
        for k in range(1, nc):
            to_ctx(k, a).start()
        for j in range(1, ns):
            to_shard(0, j, a).start()

    local = [pltpu.make_async_copy(x_ref, X.at[:, pl.ds(HALO, length), columns(z)], lsem.at[0])]
    local += [
        pltpu.make_async_copy(array[0], rows(array, s, c), lsem.at[1 + a])
        for a, array in enumerate(arrays)
    ]
    for copy in local:
        copy.start()

    @pl.when(c == 0)
    def _():
        hv[...] = jnp.zeros_like(hv)

    @pl.when(c > 0)
    def _():
        remote(hv, hv, hs, hr, ctx=lax.rem(c + nc - 1, nc)).wait_recv()

    @pl.when(z < nz - 1)
    def _():
        up(0, count).start()

    @pl.when(z > 0)
    def _():
        down(0, count).start()

    halo_copy = pltpu.make_async_copy(hv, X.at[:, pl.ds(0, HALO), columns(z)], lsem.at[4])
    halo_copy.start()

    for d in range(1, nz):
        for i in range(count + 1):

            @pl.when(z - d >= 0)
            def _():
                got_up(d, i).wait_recv()
                if d < nz - 1:

                    @pl.when(z < nz - 1)
                    def _():
                        up(d, i).start()

            @pl.when(z + d < nz)
            def _():
                got_down(d, i).wait_recv()
                if d < nz - 1:

                    @pl.when(z > 0)
                    def _():
                        down(d, i).start()

        if d == max(1, nz - 2):
            for a in range(3):
                for k in range(1, nc):
                    from_ctx(k, a).wait_recv()
                    for j in range(1, ns):
                        to_shard(k, j, a).start()

    for a in range(3):
        for k in range(nc):
            for j in range(1, ns):
                from_shard(k, j, a).wait_recv()
    for copy in local:
        copy.wait()
    halo_copy.wait()

    @pl.when(c < nc - 1)
    def _():
        halo_send.wait_send()

    for d in range(nz - 1):
        for i in range(count + 1):

            @pl.when((z - d >= 0) & (z < nz - 1))
            def _():
                up(d, i).wait_send()

            @pl.when((z + d < nz) & (z > 0))
            def _():
                down(d, i).wait_send()

    for a in range(3):
        for k in range(1, nc):
            to_ctx(k, a).wait_send()
        for k in range(nc):
            for j in range(1, ns):
                to_shard(k, j, a).wait_send()


def gather(x, gv, ow, sw):
    ns, nc, nz = dims = sizes()
    seqs, length, quarter = x.shape
    shapes = [(seqs, length + HALO, quarter * nz)] + [(w.shape[0] * ns * nc, w.shape[1]) for w in (gv, ow, sw)]
    parts = 2 * seqs + 1
    dma = pltpu.SemaphoreType.DMA
    return pl.pallas_call(
        functools.partial(gather_kernel, dims),
        out_shape=[jax.ShapeDtypeStruct(shape, BF16) for shape in shapes],
        in_specs=[vmem_spec()] * 4,
        out_specs=[any_spec()] * 4,
        scratch_shapes=[
            pltpu.VMEM((seqs, HALO, quarter), BF16),
            dma((5,)),
            dma,
            dma,
            dma((2, nz - 1, parts)),
            dma((2, nz - 1, parts)),
            dma((nc - 1, 3)),
            dma((nc - 1, 3)),
            dma((nc, ns - 1, 3)),
            dma((nc, ns - 1, 3)),
        ],
        compiler_params=pltpu.CompilerParams(
            collective_id=0, has_side_effects=True, vmem_limit_bytes=VMEM_ALL
        ),
        name="gather",
    )(x, gv, ow, sw)


def project_kernel(x_ref, gain_ref, gv_ref, sw_ref, normed_ref, out_ref, small_ref, scale_ref):
    u = x_ref[0].astype(F32)
    scale = lax.rsqrt(jnp.mean(u * u, axis=1, keepdims=True) + EPSILON)
    normed = (u * scale * gain_ref[...]).astype(BF16)
    normed_ref[0] = normed
    scale_ref[0] = jnp.broadcast_to(scale, scale_ref.shape[1:])
    out_ref[0] = dot_nn(normed, gv_ref[...]).astype(BF16)
    small_ref[0] = dot_nn(normed, sw_ref[...])


def project(X, gain, GV, SW):
    seqs, rows, width = X.shape
    block = rows // 3
    full = lambda array: pl.BlockSpec(array.shape, lambda q, r: (0, 0))
    tile = lambda cols: pl.BlockSpec((1, block, cols), lambda q, r: (q, r, 0))
    return pl.pallas_call(
        project_kernel,
        grid=(seqs, 3),
        in_specs=[tile(width), full(gain), full(GV), full(SW)],
        out_specs=[tile(width), tile(GV.shape[1]), tile(SW.shape[1]), tile(LANES)],
        out_shape=[
            jax.ShapeDtypeStruct((seqs, rows, width), BF16),
            jax.ShapeDtypeStruct((seqs, rows, GV.shape[1]), BF16),
            jax.ShapeDtypeStruct((seqs, rows, SW.shape[1]), F32),
            jax.ShapeDtypeStruct((seqs, rows, LANES), F32),
        ],
        compiler_params=pltpu.CompilerParams(vmem_limit_bytes=VMEM_ALL),
        name="project",
    )(X, gain, GV, SW)


def sigmoid(value):
    return 1.0 / (1.0 + jnp.exp(-value))


def iota(axis, shape=(CHUNK, LANES)):
    return lax.broadcasted_iota(jnp.int32, shape, axis)


def causal_conv(padded, taps, bias):
    width = taps.shape[0]
    total = bias + taps[width - 1 : width] * padded[HALO:]
    for offset in range(width - 1):
        shifted = pltpu.roll(padded, width - 1 - offset, 0)
        total = total + taps[offset : offset + 1] * shifted[HALO:]
    return total


def conv_back(padded, taps, rows):
    width = taps.shape[0]
    total = taps[width - 1 : width] * padded[:rows]
    for offset in range(width - 1):
        ahead = width - 1 - offset
        shifted = pltpu.roll(padded, padded.shape[0] - ahead, 0)
        total = total + taps[offset : offset + 1] * shifted[:rows]
    return total


def pair(columns, p):
    rows = columns.shape[0]
    first = iota(1, (rows, LANES)) < LANES // 2
    left = jnp.broadcast_to(columns[:, 2 * p : 2 * p + 1], (rows, LANES))
    right = jnp.broadcast_to(columns[:, 2 * p + 1 : 2 * p + 2], (rows, LANES))
    return jnp.where(first, left, right)


def stacked(value):
    first = iota(1, value.shape) < LANES // 2
    zero = jnp.zeros_like(value)
    both = [jnp.where(first, value, zero), jnp.where(first, zero, value)]
    return jnp.concatenate(both, axis=0).astype(BF16)


def head_sums(p):
    rows, cols = iota(0, (LANES, LANES)), iota(1, (LANES, LANES))
    return jnp.where(cols == 2 * p + jnp.where(rows < LANES // 2, 0, 1), 1.0, 0.0)


def softplus(value):
    return jnp.maximum(value, 0.0) + jnp.log1p(jnp.exp(-jnp.abs(value)))


def join_states(own_ref, decay_ref, mine, backward, q):
    count = own_ref.shape[0]
    total = jnp.zeros(own_ref.shape[2:], F32)
    for step in range(count):
        i = count - 1 - step if backward else step
        longer = decay_ref[i, q, 0:1, :] * total + own_ref[i, q].astype(F32)
        total = jnp.where((mine < i) if backward else (i < mine), longer, total)
    return total


def forward_kernel(
    heads,
    gv_ref,
    small_ref,
    vk_ref,
    vb_ref,
    mk_ref,
    mb_ref,
    sb_ref,
    rate_ref,
    v_ref,
    slope_ref,
    y_ref,
    starts_ref,
    own_ref,
    step_ref,
    cum_ref,
    carry_ref,
    mat_ref,
    mslope_ref,
    end_ref,
    state,
    carry,
):
    k = pl.program_id(1)

    @pl.when(k == 0)
    def _():
        state[...] = jnp.zeros_like(state)
        carry[...] = jnp.zeros_like(carry)

    rows = pl.ds(pl.multiple_of(k * CHUNK, CHUNK), CHUNK + HALO)
    small = small_ref[0, rows, :]
    mwidth = mk_ref.shape[1]
    matrix_in = small[:, :mwidth].astype(BF16).astype(F32)
    mconv = causal_conv(matrix_in, mk_ref[...], mb_ref[...])
    msig = sigmoid(mconv)
    mat = mconv * msig
    mat_ref[0] = mat
    mslope_ref[0] = msig * (1.0 + mconv * (1.0 - msig))
    b_mat, c_mat = mat[:, : mwidth // 2], mat[:, mwidth // 2 :]
    b_low, c_low = b_mat.astype(BF16), c_mat.astype(BF16)
    bt_low = b_mat.T.astype(BF16)
    gram = dot_nt(c_low, b_low)

    lane = iota(1)
    raw = small[HALO:, mwidth:] + sb_ref[...]
    step = jnp.where(lane < heads, softplus(raw), 0.0)
    tri = jnp.where(iota(0) >= lane, 1.0, 0.0)
    cum = dot_nn(tri, step * rate_ref[...], HIGHEST)
    cum_t = cum.T
    step_ref[0] = step
    cum_ref[0] = cum
    carry_ref[0, 0] = carry[...]
    last = cum[CHUNK - 1 : CHUNK, :]
    carry[...] = carry[...] + last
    from_start = jnp.exp(cum)
    to_end = jnp.exp(last - cum)
    whole = jnp.exp(last)
    causal = iota(0) >= lane

    for p in range(heads // 2):
        cols = slice(p * LANES, (p + 1) * LANES)
        signal = gv_ref[0, rows, cols].astype(F32)
        conv = causal_conv(signal, vk_ref[:, cols], vb_ref[:, cols])
        sig = sigmoid(conv)
        v = conv * sig
        v_ref[0, :, cols] = v
        slope_ref[0, :, cols] = sig * (1.0 + conv * (1.0 - sig))
        scaled = v * pair(step, p)
        weights = []
        for h in (2 * p, 2 * p + 1):
            spread = cum[:, h : h + 1] - cum_t[h : h + 1, :]
            weights.append(jnp.where(causal, jnp.exp(spread) * gram, 0.0))
        weights = jnp.concatenate(weights, axis=1).astype(BF16)
        old = state[:, cols]
        starts_ref[0, 0, :, cols] = old
        y = dot_nn(weights, stacked(scaled))
        y = y + pair(from_start, p) * dot_nn(c_low, old.astype(BF16))
        y_ref[0, :, cols] = y
        new = dot_nn(bt_low, (scaled * pair(to_end, p)).astype(BF16))
        state[:, cols] = pair(whole, p) * old + new

    @pl.when(k == pl.num_programs(1) - 1)
    def _():
        own_ref[0] = state[...].astype(own_ref.dtype)
        end = jnp.exp(carry[...])
        for p in range(heads // 2):
            end_ref[0, :, p * LANES : (p + 1) * LANES] = pair(end, p)


def forward(gate_value, small, vk, vb, mk, mb, sb, rate, heads):
    seqs, rows, width = gate_value.shape
    inner = width // 2
    length = rows - HALO
    chunks = length // CHUNK
    state_width = mk.shape[1] // 2
    full = lambda array: pl.BlockSpec(array.shape, lambda q, k: (0, 0))
    tile = lambda cols: pl.BlockSpec((1, CHUNK, cols), lambda q, k: (q, k, 0))
    out = [
        ((seqs, length, inner), F32, tile(inner)),
        ((seqs, length, inner), F32, tile(inner)),
        ((seqs, length, inner), F32, tile(inner)),
        (
            (seqs, chunks, state_width, inner),
            F32,
            pl.BlockSpec((1, 1, state_width, inner), lambda q, k: (q, k, 0, 0)),
        ),
        (
            (seqs, state_width, inner),
            F32 if FINE_S else BF16,
            pl.BlockSpec((1, state_width, inner), lambda q, k: (q, 0, 0)),
        ),
        ((seqs, length, LANES), F32, tile(LANES)),
        ((seqs, length, LANES), F32, tile(LANES)),
        ((seqs, chunks, 8, LANES), F32, pl.BlockSpec((1, 1, 8, LANES), lambda q, k: (q, k, 0, 0))),
        ((seqs, length, 2 * state_width), F32, tile(2 * state_width)),
        ((seqs, length, 2 * state_width), F32, tile(2 * state_width)),
        ((seqs, 8, inner), F32, pl.BlockSpec((1, 8, inner), lambda q, k: (q, 0, 0))),
    ]
    return pl.pallas_call(
        functools.partial(forward_kernel, heads),
        grid=(seqs, chunks),
        in_specs=[
            pl.BlockSpec((1, rows, inner), lambda q, k: (q, 0, 1)),
            pl.BlockSpec((1, rows, small.shape[2]), lambda q, k: (q, 0, 0)),
        ]
        + [full(array) for array in (vk, vb, mk, mb, sb, rate)],
        out_specs=[spec for _, _, spec in out],
        out_shape=[jax.ShapeDtypeStruct(shape, dtype) for shape, dtype, _ in out],
        scratch_shapes=[pltpu.VMEM((state_width, inner), F32), pltpu.VMEM((8, LANES), F32)],
        compiler_params=pltpu.CompilerParams(vmem_limit_bytes=VMEM_ALL),
        name="forward",
    )(gate_value, small, vk, vb, mk, mb, sb, rate)


def exchange_kernel(dims, backward, own_ref, end_ref, all_ref, ends_ref, lsem, ss, sr, es, er):
    ns, nc, nz = dims
    s, c, z = places()
    greet([(None, {"ctx": lax.rem(c + k, nc)}) for k in range(1, nc)], nc - 1)

    def state(k):
        there = c - k if backward else c + k
        return remote(
            own_ref, all_ref.at[c], ss.at[k - 1], sr.at[k - 1], ctx=lax.rem(there + nc, nc)
        )

    def arrived(k):
        owner = lax.rem((c + k if backward else c - k) + nc, nc)
        return remote(own_ref, all_ref.at[owner], ss.at[k - 1], sr.at[k - 1], ctx=owner)

    def ends(k):
        return remote(
            end_ref, ends_ref.at[c], es.at[k - 1], er.at[k - 1], ctx=lax.rem(c + k, nc)
        )

    def ends_arrived(k):
        owner = lax.rem(c + nc - k, nc)
        return remote(end_ref, ends_ref.at[owner], es.at[k - 1], er.at[k - 1], ctx=owner)

    def sends(k):
        return (c - k >= 0) if backward else (c + k < nc)

    def receives(k):
        return (c + k < nc) if backward else (c - k >= 0)

    for k in range(1, nc):

        @pl.when(sends(k))
        def _():
            state(k).start()

        if not backward:
            ends(k).start()
    copies = [pltpu.make_async_copy(own_ref, all_ref.at[c], lsem.at[0])]
    if not backward:
        copies.append(pltpu.make_async_copy(end_ref, ends_ref.at[c], lsem.at[1]))
    for copy in copies:
        copy.start()
    for k in range(1, nc):

        @pl.when(receives(k))
        def _():
            arrived(k).wait_recv()

        if not backward:
            ends_arrived(k).wait_recv()
    for copy in copies:
        copy.wait()
    for k in range(1, nc):

        @pl.when(sends(k))
        def _():
            state(k).wait_send()

        if not backward:
            ends(k).wait_send()


def exchange(own, end, backward):
    ns, nc, nz = dims = sizes()
    dma = pltpu.SemaphoreType.DMA
    return pl.pallas_call(
        functools.partial(exchange_kernel, dims, backward),
        out_shape=[
            jax.ShapeDtypeStruct((nc,) + own.shape, own.dtype),
            jax.ShapeDtypeStruct((nc,) + end.shape, end.dtype),
        ],
        in_specs=[vmem_spec()] * 2,
        out_specs=[any_spec()] * 2,
        scratch_shapes=[dma((2,))] + [dma((nc - 1,))] * 4,
        compiler_params=pltpu.CompilerParams(
            collective_id=2 if backward else 1, has_side_effects=True
        ),
        name="adjoints" if backward else "states",
    )(own, end)


def gate_kernel(
    heads,
    y_ref,
    v_ref,
    gv_ref,
    cot_ref,
    ow_ref,
    cum_ref,
    carry_ref,
    mat_ref,
    all_ref,
    ends_ref,
    ig_ref,
    skip_ref,
    ssd_ref,
    grad_inner_ref,
    sums_ref,
    start_ref,
):
    q, k = pl.program_id(0), pl.program_id(1)

    @pl.when(k == 0)
    def _():
        start_ref[0] = join_states(all_ref, ends_ref, lax.axis_index("ctx"), False, 0)

    rows = pl.ds(pl.multiple_of(HALO + k * CHUNK, HALO), CHUNK)
    half = mat_ref.shape[2] // 2
    c_low = mat_ref[0, :, half:].astype(BF16)
    from_start = jnp.exp(cum_ref[0] + carry_ref[0, 0, 0:1, :])
    grad_inner = dot_nn(cot_ref[0], ow_ref[...])
    grad_inner_ref[0] = grad_inner
    squares = jnp.zeros((CHUNK, LANES), F32)
    dots = jnp.zeros((CHUNK, LANES), F32)
    for p in range(heads // 2):
        cols = slice(p * LANES, (p + 1) * LANES)
        carried = dot_nn(c_low, start_ref[0, :, cols].astype(BF16))
        ssd = y_ref[0, :, cols] + pair(from_start, p) * carried
        ssd_ref[0, :, cols] = ssd
        gate = gv_ref[0, rows, cols].astype(F32)
        mixed = ssd + skip_ref[:, cols] * v_ref[0, :, cols]
        gated = mixed * (gate * sigmoid(gate))
        squares = squares + gated * gated
        dots = dots + grad_inner[:, cols] * ig_ref[:, cols] * gated
    ones = jnp.ones((8, LANES), F32)
    first = iota(0, (8, CHUNK)) == 0
    sums_ref[0] = jnp.where(first, dot_nt(ones, squares, HIGHEST), dot_nt(ones, dots, HIGHEST))


def gate_step(y, v, gate_value, cot, OW, cum, carry, mat, all_states, ends, ig, skip, heads):
    seqs, length, inner = y.shape
    rows = gate_value.shape[1]
    chunks = length // CHUNK
    count, _, state_width, _ = all_states.shape
    width = cot.shape[2]
    full = lambda array: pl.BlockSpec(array.shape, lambda q, k: (0, 0))
    tile = lambda cols: pl.BlockSpec((1, CHUNK, cols), lambda q, k: (q, k, 0))
    return pl.pallas_call(
        functools.partial(gate_kernel, heads),
        grid=(seqs, chunks),
        in_specs=[
            tile(inner),
            tile(inner),
            pl.BlockSpec((1, rows, inner), lambda q, k: (q, 0, 0)),
            tile(width),
            full(OW),
            tile(LANES),
            pl.BlockSpec((1, 1, 8, LANES), lambda q, k: (q, k, 0, 0)),
            tile(2 * state_width),
            pl.BlockSpec((count, 1, state_width, inner), lambda q, k: (0, q, 0, 0)),
            pl.BlockSpec((count, 1, 8, inner), lambda q, k: (0, q, 0, 0)),
            full(ig),
            full(skip),
        ],
        out_specs=[
            tile(inner),
            tile(inner),
            pl.BlockSpec((1, 8, CHUNK), lambda q, k: (q, 0, k)),
            pl.BlockSpec((1, state_width, inner), lambda q, k: (q, 0, 0)),
        ],
        out_shape=[
            jax.ShapeDtypeStruct((seqs, length, inner), F32),
            jax.ShapeDtypeStruct((seqs, length, inner), F32),
            jax.ShapeDtypeStruct((seqs, 8, length), F32),
            jax.ShapeDtypeStruct((seqs, state_width, inner), F32),
        ],
        compiler_params=pltpu.CompilerParams(vmem_limit_bytes=VMEM_ALL),
        name="gates",
    )(y, v, gate_value, cot, OW, cum, carry, mat, all_states, ends, ig, skip)


def token_sum_kernel(dims, own_ref, total_ref, slots, ss, sr):
    ns, nc, nz = dims
    s, c, z = places()
    greet([(None, {"tensor": lax.rem(z + k, nz)}) for k in range(1, nz)], nz - 1)

    def send(k):
        return remote(
            own_ref, slots.at[k - 1], ss.at[k - 1], sr.at[k - 1], tensor=lax.rem(z + k, nz)
        )

    for k in range(1, nz):
        send(k).start()
    total = own_ref[...]
    for k in range(1, nz):
        send(k).wait_recv()
        total = total + slots[k - 1]
    total_ref[...] = total
    for k in range(1, nz):
        send(k).wait_send()


def token_sum(own):
    ns, nc, nz = dims = sizes()
    dma = pltpu.SemaphoreType.DMA
    return pl.pallas_call(
        functools.partial(token_sum_kernel, dims),
        out_shape=jax.ShapeDtypeStruct(own.shape, F32),
        in_specs=[vmem_spec()],
        out_specs=vmem_spec(),
        scratch_shapes=[pltpu.VMEM((nz - 1,) + own.shape, F32)] + [dma((nz - 1,))] * 2,
        compiler_params=pltpu.CompilerParams(collective_id=3, has_side_effects=True),
        name="token_sum",
    )(own)


def mixed_kernel(
    heads,
    inner_total,
    ssd_ref,
    v_ref,
    gv_ref,
    grad_inner_ref,
    sums_ref,
    ow_ref,
    cum_ref,
    carry_ref,
    mat_ref,
    ig_ref,
    skip_ref,
    gm_ref,
    gate_ref,
    inner_ref,
    part_ref,
    adjoint_ref,
    vec_ref,
    total,
):
    q, k = pl.program_id(0), pl.program_id(1)

    @pl.when(k == 0)
    def _():
        total[...] = jnp.zeros_like(total)
        gate_ref[0, 0:HALO, :] = jnp.zeros((HALO, gate_ref.shape[2]), BF16)

    @pl.when((k == 0) & (q == 0))
    def _():
        vec_ref[...] = jnp.zeros_like(vec_ref)

    rows = pl.ds(pl.multiple_of(HALO + k * CHUNK, HALO), CHUNK)
    half = mat_ref.shape[2] // 2
    ct_low = mat_ref[0, :, half:].T.astype(BF16)
    from_start = jnp.exp(cum_ref[0] + carry_ref[0, 0, 0:1, :])
    sums = sums_ref[0].T
    scale = lax.rsqrt(sums[:, 0:1] / inner_total + EPSILON)
    row_dot = sums[:, 1:2] / inner_total
    scale = jnp.broadcast_to(scale, (CHUNK, LANES))
    back = scale * scale * scale * jnp.broadcast_to(row_dot, (CHUNK, LANES))
    for p in range(heads // 2):
        cols = slice(p * LANES, (p + 1) * LANES)
        v = v_ref[0, :, cols]
        mixed = ssd_ref[0, :, cols] + skip_ref[:, cols] * v
        gate = gv_ref[0, rows, cols].astype(F32)
        sig = sigmoid(gate)
        act = gate * sig
        gated = mixed * act
        grad_inner = grad_inner_ref[0, :, cols]
        normal = gated * scale
        inner_ref[0, :, cols] = (normal * ig_ref[:, cols]).astype(BF16)
        grad_gated = scale * (grad_inner * ig_ref[:, cols]) - gated * back
        grad_mixed = grad_gated * act
        gm_ref[0, :, cols] = grad_mixed
        slope = sig * (1.0 + gate * (1.0 - sig))
        gate_ref[0, rows, cols] = (grad_gated * mixed * slope).astype(BF16)
        vec_ref[0:1, cols] += jnp.sum(grad_inner * normal, axis=0, keepdims=True)
        vec_ref[1:2, cols] += jnp.sum(grad_mixed * v, axis=0, keepdims=True)
        total[:, cols] += dot_nn(ct_low, (grad_mixed * pair(from_start, p)).astype(BF16))
    quarter = part_ref.shape[3]
    for j in range(part_ref.shape[0]):
        rows_of = slice(j * quarter, (j + 1) * quarter)
        part_ref[j, 0] = dot_nt(inner_ref[0], ow_ref[rows_of, :]).astype(BF16)

    @pl.when(k == pl.num_programs(1) - 1)
    def _():
        adjoint_ref[0] = total[...].astype(adjoint_ref.dtype)


def mixed_step(
    ssd, v, gate_value, grad_inner, sums, OW, cum, carry, mat, ig, skip, heads, inner_total, nz
):
    seqs, length, inner = ssd.shape
    rows = gate_value.shape[1]
    chunks = length // CHUNK
    state_width = mat.shape[2] // 2
    width = OW.shape[0]
    full = lambda array: pl.BlockSpec(array.shape, lambda q, k: (0, 0))
    tile = lambda cols: pl.BlockSpec((1, CHUNK, cols), lambda q, k: (q, k, 0))
    return pl.pallas_call(
        functools.partial(mixed_kernel, heads, inner_total),
        grid=(seqs, chunks),
        in_specs=[
            tile(inner),
            tile(inner),
            pl.BlockSpec((1, rows, inner), lambda q, k: (q, 0, 0)),
            tile(inner),
            pl.BlockSpec((1, 8, CHUNK), lambda q, k: (q, 0, k)),
            full(OW),
            tile(LANES),
            pl.BlockSpec((1, 1, 8, LANES), lambda q, k: (q, k, 0, 0)),
            tile(2 * state_width),
            full(ig),
            full(skip),
        ],
        out_specs=[
            tile(inner),
            pl.BlockSpec((1, rows, inner), lambda q, k: (q, 0, 0)),
            tile(inner),
            pl.BlockSpec((nz, 1, CHUNK, width // nz), lambda q, k: (0, q, k, 0)),
            pl.BlockSpec((1, state_width, inner), lambda q, k: (q, 0, 0)),
            pl.BlockSpec((8, inner), lambda q, k: (0, 0)),
        ],
        out_shape=[
            jax.ShapeDtypeStruct((seqs, length, inner), F32),
            jax.ShapeDtypeStruct((seqs, rows, inner), BF16),
            jax.ShapeDtypeStruct((seqs, length, inner), BF16),
            jax.ShapeDtypeStruct((nz, seqs, length, width // nz), BF16),
            jax.ShapeDtypeStruct((seqs, state_width, inner), F32 if FINE_S else BF16),
            jax.ShapeDtypeStruct((8, inner), F32),
        ],
        scratch_shapes=[pltpu.VMEM((state_width, inner), F32)],
        compiler_params=pltpu.CompilerParams(vmem_limit_bytes=VMEM_ALL),
        name="mixed",
    )(ssd, v, gate_value, grad_inner, sums, OW, cum, carry, mat, ig, skip)


def backward_kernel(
    heads,
    gm_ref,
    v_ref,
    slope_ref,
    ssd_ref,
    starts_ref,
    carry_ref,
    cum_ref,
    step_ref,
    mat_ref,
    mslope_ref,
    start_ref,
    all_ref,
    ends_ref,
    gv_ref,
    small_ref,
    vk_ref,
    mk_ref,
    sb_ref,
    rate_ref,
    skip_ref,
    gx_ref,
    gs_ref,
    vec_ref,
    mvec_ref,
    svec_ref,
    incoming,
    ahead,
    mahead,
    step_dot,
    cum_grad,
    mixing,
    grad_b,
    grad_c,
    log_start,
):
    q, k = pl.program_id(0), pl.program_id(1)
    chunks = pl.num_programs(1)
    chunk = chunks - 1 - k
    mwidth = mk_ref.shape[1]
    half = mwidth // 2

    @pl.when(k == 0)
    def _():
        incoming[...] = join_states(all_ref, ends_ref, lax.axis_index("ctx"), True, 0)
        ahead[...] = jnp.zeros_like(ahead)
        mahead[...] = jnp.zeros_like(mahead)

    @pl.when((k == 0) & (q == 0))
    def _():
        vec_ref[...] = jnp.zeros_like(vec_ref)
        mvec_ref[...] = jnp.zeros_like(mvec_ref)
        svec_ref[...] = jnp.zeros_like(svec_ref)

    padded = pl.ds(pl.multiple_of(chunk * CHUNK, CHUNK), CHUNK + HALO)
    rows = pl.ds(pl.multiple_of(HALO + chunk * CHUNK, HALO), CHUNK)
    mat = mat_ref[0]
    b_mat, c_mat = mat[:, :half], mat[:, half:]
    b_low, c_low = b_mat.astype(BF16), c_mat.astype(BF16)
    ct_low = c_mat.T.astype(BF16)
    gram_t = dot_nt(b_low, c_low)
    step = step_ref[0]
    cum = cum_ref[0]
    cum_t = cum.T
    last = cum[CHUNK - 1 : CHUNK, :]
    from_start = jnp.exp(cum)
    to_end = jnp.exp(last - cum)
    whole = jnp.exp(last)
    before = jnp.exp(carry_ref[0, 0, 0:1, :])
    lane = iota(1)
    later = lane >= iota(0)

    step_dot[...] = jnp.zeros_like(step_dot)
    cum_grad[...] = jnp.zeros_like(cum_grad)
    mixing[...] = jnp.zeros_like(mixing)
    grad_b[...] = jnp.zeros_like(grad_b)
    grad_c[...] = jnp.zeros_like(grad_c)
    log_start[...] = jnp.zeros_like(log_start)

    for p in range(heads // 2):
        cols = slice(p * LANES, (p + 1) * LANES)
        gm = gm_ref[0, :, cols]
        v = v_ref[0, :, cols]
        stepped = pair(step, p)
        scaled = v * stepped
        gm_low, gm_rest = split(gm)
        scaled_low, scaled_rest = split(scaled)
        both = stacked(scaled_low.astype(F32))
        products = dot_nt(both, gm_low)
        if FINE_A:
            products = products + dot_nt(both, gm_rest)
            products = products + dot_nt(stacked(scaled_rest.astype(F32)), gm_low)
        weights = []
        mix = mixing[...]
        for i, h in enumerate((2 * p, 2 * p + 1)):
            spread = cum_t[h : h + 1, :] - cum[:, h : h + 1]
            decay = jnp.where(later, jnp.exp(spread), 0.0)
            weights.append(decay * gram_t)
            mix = mix + decay * products[i * CHUNK : (i + 1) * CHUNK]
        mixing[...] = mix
        weights = jnp.concatenate(weights, axis=1).astype(BF16)
        inc = incoming[:, cols]
        inc_low = inc.astype(BF16)
        ended = pair(to_end, p)
        b_dot = dot_nn(weights, stacked(gm)) + ended * dot_nn(b_low, inc_low)
        begun = gm * pair(from_start, p)
        begun_low = begun.astype(BF16)
        start = starts_ref[0, 0, :, cols] + pair(before, p) * start_ref[0, :, cols]
        if FINE_B:
            grad_b[...] += fine(dot_nt, scaled * ended, inc)
            grad_c[...] += fine(dot_nt, begun, start)
        else:
            grad_b[...] += dot_nt((scaled * ended).astype(BF16), inc_low)
            grad_c[...] += dot_nt(begun_low, start.astype(BF16))
        earlier = pair(whole, p) * inc + dot_nn(ct_low, begun_low)
        incoming[:, cols] = earlier
        heads_of = head_sums(p)
        log_start[...] += dot_nn(
            jnp.broadcast_to(jnp.sum(earlier * start, axis=0, keepdims=True), (8, LANES)),
            heads_of,
            HIGHEST,
        )
        step_dot[...] += dot_nn(v * b_dot, heads_of, HIGHEST)
        cum_grad[...] += dot_nn(
            gm_low.astype(F32) * ssd_ref[0, :, cols] - scaled.astype(BF16).astype(F32) * b_dot,
            heads_of,
            HIGHEST,
        )
        conv_grad = (stepped * b_dot + skip_ref[:, cols] * gm) * slope_ref[0, :, cols]
        taps = vk_ref[:, cols]
        width = taps.shape[0]
        signal = gv_ref[0, padded, cols].astype(F32)
        for offset in range(width):
            moved = signal if offset == width - 1 else pltpu.roll(signal, width - 1 - offset, 0)
            vec_ref[offset : offset + 1, cols] += jnp.sum(
                conv_grad * moved[HALO:], axis=0, keepdims=True
            )
        vec_ref[width : width + 1, cols] += jnp.sum(conv_grad, axis=0, keepdims=True)
        extended = jnp.concatenate([conv_grad, ahead[:, cols]], axis=0)
        gx_ref[0, rows, cols] = conv_back(extended, taps, CHUNK).astype(BF16)
        ahead[:, cols] = conv_grad[:HALO]

        @pl.when(chunk == 0)
        def _():
            front = jnp.concatenate([jnp.zeros((HALO, LANES), F32), conv_grad[:HALO]], axis=0)
            gx_ref[0, 0:HALO, cols] = conv_back(front, taps, HALO).astype(BF16)

    mix = mixing[...]
    if FINE_C:
        total_b = grad_b[...] + fine(dot_nn, mix, c_mat)
        total_c = grad_c[...] + fine(dot_nn, mix.T, b_mat)
    else:
        total_b = grad_b[...] + dot_nn(mix.astype(BF16), c_low)
        total_c = grad_c[...] + dot_nn(mix.T.astype(BF16), b_low)
    mgrad = jnp.concatenate([total_b, total_c], axis=1) * mslope_ref[0]
    mtaps = mk_ref[...]
    width = mtaps.shape[0]
    small = small_ref[0, padded, :]
    signal = small[:, :mwidth].astype(BF16).astype(F32)
    for offset in range(width):
        moved = signal if offset == width - 1 else pltpu.roll(signal, width - 1 - offset, 0)
        mvec_ref[offset : offset + 1, :] += jnp.sum(mgrad * moved[HALO:], axis=0, keepdims=True)
    mvec_ref[width : width + 1, :] += jnp.sum(mgrad, axis=0, keepdims=True)
    extended = jnp.concatenate([mgrad, mahead[...]], axis=0)
    gs_ref[0, rows, 0:mwidth] = conv_back(extended, mtaps, CHUNK).astype(BF16)
    mahead[...] = mgrad[:HALO]

    earlier_only = jnp.where(lane < iota(0), 1.0, 0.0)
    value_dot = step_dot[...]
    grad_log = log_start[0:1, :] - dot_nn(earlier_only, cum_grad[...], HIGHEST)
    grad_log = jnp.where(lane < heads, grad_log, 0.0)
    grad_step = value_dot + grad_log * rate_ref[...]
    raw = small[HALO:, mwidth:] + sb_ref[...]
    grad_raw = jnp.where(lane < heads, grad_step * sigmoid(raw), 0.0)
    svec_ref[0:1, :] += jnp.sum(grad_raw, axis=0, keepdims=True)
    svec_ref[1:2, :] += jnp.sum(grad_log * step, axis=0, keepdims=True)
    gs_ref[0, rows, mwidth:] = grad_raw.astype(BF16)

    @pl.when(chunk == 0)
    def _():
        front = jnp.concatenate([jnp.zeros((HALO, mwidth), F32), mgrad[:HALO]], axis=0)
        gs_ref[0, 0:HALO, 0:mwidth] = conv_back(front, mtaps, HALO).astype(BF16)
        gs_ref[0, 0:HALO, mwidth:] = jnp.zeros((HALO, gs_ref.shape[2] - mwidth), BF16)


def backward(
    gm, v, slope, ssd, starts, carry, cum, step, mat, mslope, start, adjoints, ends,
    gate_value, small, vk, mk, sb, rate, skip, heads,
):
    seqs, length, inner = gm.shape
    rows = gate_value.shape[1]
    chunks = length // CHUNK
    state_width = mat.shape[2] // 2
    count = adjoints.shape[0]
    swidth = small.shape[2]
    full = lambda array: pl.BlockSpec(array.shape, lambda q, k: (0, 0))
    tile = lambda cols: pl.BlockSpec((1, CHUNK, cols), lambda q, k: (q, chunks - 1 - k, 0))
    whole = lambda height, cols, at=0: pl.BlockSpec((1, height, cols), lambda q, k: (q, 0, at))
    every = lambda height, cols: pl.BlockSpec((count, 1, height, cols), lambda q, k: (0, q, 0, 0))
    return pl.pallas_call(
        functools.partial(backward_kernel, heads),
        grid=(seqs, chunks),
        in_specs=[
            tile(inner),
            tile(inner),
            tile(inner),
            tile(inner),
            pl.BlockSpec((1, 1, state_width, inner), lambda q, k: (q, chunks - 1 - k, 0, 0)),
            pl.BlockSpec((1, 1, 8, LANES), lambda q, k: (q, chunks - 1 - k, 0, 0)),
            tile(LANES),
            tile(LANES),
            tile(2 * state_width),
            tile(2 * state_width),
            whole(state_width, inner),
            every(state_width, inner),
            every(8, inner),
            whole(rows, inner, 1),
            whole(rows, swidth),
            full(vk),
            full(mk),
            full(sb),
            full(rate),
            full(skip),
        ],
        out_specs=[
            whole(rows, inner),
            whole(rows, swidth),
            pl.BlockSpec((8, inner), lambda q, k: (0, 0)),
            pl.BlockSpec((8, 2 * state_width), lambda q, k: (0, 0)),
            pl.BlockSpec((8, LANES), lambda q, k: (0, 0)),
        ],
        out_shape=[
            jax.ShapeDtypeStruct((seqs, rows, inner), BF16),
            jax.ShapeDtypeStruct((seqs, rows, swidth), BF16),
            jax.ShapeDtypeStruct((8, inner), F32),
            jax.ShapeDtypeStruct((8, 2 * state_width), F32),
            jax.ShapeDtypeStruct((8, LANES), F32),
        ],
        scratch_shapes=[
            pltpu.VMEM((state_width, inner), F32),
            pltpu.VMEM((HALO, inner), F32),
            pltpu.VMEM((HALO, 2 * state_width), F32),
        ]
        + [pltpu.VMEM((CHUNK, LANES), F32)] * 5
        + [pltpu.VMEM((8, LANES), F32)],
        compiler_params=pltpu.CompilerParams(vmem_limit_bytes=VMEM_ALL),
        name="backward",
    )(
        gm, v, slope, ssd, starts, carry, cum, step, mat, mslope, start, adjoints, ends,
        gate_value, small, vk, mk, sb, rate, skip,
    )


def normed_kernel(blocks, gz_ref, gx_ref, gs_ref, normed_ref, gv_ref, sw_ref, out_ref, row_ref, col_ref, acc):
    q = pl.program_id(0)
    height = gz_ref.shape[1] // blocks
    inner = gz_ref.shape[2]
    width = out_ref.shape[2]

    @pl.when(q == 0)
    def _():
        col_ref[...] = jnp.zeros_like(col_ref)

    acc[...] = jnp.zeros_like(acc)
    for r in range(blocks):
        rows = slice(r * height, (r + 1) * height)
        part = dot_nt(gz_ref[0, rows, :], gv_ref[:, 0:inner])
        part = part + dot_nt(gx_ref[0, rows, :], gv_ref[:, inner:])
        part = part + dot_nt(gs_ref[0, rows, :], sw_ref[...])
        out_ref[0, rows, :] = part.astype(BF16)
        product = part * normed_ref[0, rows, :].astype(F32)
        col_ref[0:1, :] += jnp.sum(product, axis=0, keepdims=True)
        total = product[:, 0:LANES]
        for t in range(1, width // LANES):
            total = total + product[:, t * LANES : (t + 1) * LANES]
        acc[rows, :] = total
    row_ref[0] = dot_nt(jnp.ones((8, LANES), F32), acc[...], HIGHEST)


def normed_grad(gz, gx, gs, normed, GV, SW):
    seqs, rows, width = normed.shape
    padded = -(-rows // LANES) * LANES
    full = lambda array: pl.BlockSpec(array.shape, lambda q: (0, 0))
    tile = lambda array: pl.BlockSpec((1,) + array.shape[1:], lambda q: (q, 0, 0))
    return pl.pallas_call(
        functools.partial(normed_kernel, 3),
        grid=(seqs,),
        in_specs=[tile(gz), tile(gx), tile(gs), tile(normed), full(GV), full(SW)],
        out_specs=[
            tile(normed),
            pl.BlockSpec((1, 8, padded), lambda q: (q, 0, 0)),
            pl.BlockSpec((8, width), lambda q: (0, 0)),
        ],
        out_shape=[
            jax.ShapeDtypeStruct((seqs, rows, width), BF16),
            jax.ShapeDtypeStruct((seqs, 8, padded), F32),
            jax.ShapeDtypeStruct((8, width), F32),
        ],
        scratch_shapes=[pltpu.VMEM((padded, LANES), F32)],
        compiler_params=pltpu.CompilerParams(vmem_limit_bytes=VMEM_ALL),
        name="normed_grad",
    )(gz, gx, gs, normed, GV, SW)


def reduce_kernel(dims, mwidth, *refs):
    ns, nc, nz = dims
    s, c, z = places()
    part, rowsum, vec, zvec = refs[:4]
    grads = refs[4:8]
    out_part, out_row, out_vec, out_zvec = refs[8:12]
    out_grads = refs[12:16]
    up_buf, down_buf, halo_buf, row_buf, row_halo = refs[16:21]
    shard_bufs = refs[21:25]
    ctx_bufs = refs[25:29]
    mat_own, mat_buf, vec_c, vec_own, vec_s, zvec_c, zvec_own, zvec_s, zvec_z = refs[29:38]
    (us, ur, ds_, dr, hs, hr, rs, rr, rhs, rhr, ss, sr, cs, cr, ms, mr, vcs, vcr, vss, vsr, vzs, vzr) = refs[38:]
    seqs, rows, width = part.shape
    quarter = width // nz
    first_rows = rows // 2 // HALO * HALO + (HALO if (rows // HALO) % 2 else 0)
    spans = [(0, first_rows), (first_rows, rows - first_rows)]
    parts = [(q, r0, n) for q in range(seqs) for r0, n in spans]

    peers = [(None, {"tensor": lax.rem(z + k, nz)}) for k in range(1, nz)]
    peers += [(None, {"ctx": lax.rem(c + k, nc)}) for k in range(1, nc)]
    peers += [(None, {"shard": lax.rem(s + j, ns)}) for j in range(1, ns)]
    greet(peers, (nz - 1) + (nc - 1) + (ns - 1))

    def own(i, j):
        q, r0, n = parts[i]
        return part.at[q, pl.ds(r0, n), pl.ds(j * quarter, quarter)]

    def slot(buf, i, j):
        q, r0, n = parts[i]
        return buf.at[j, q, pl.ds(r0, n), :]

    def up(i, j, first):
        src = own(i, j) if first else slot(up_buf, i, j)
        return remote(src, slot(up_buf, i, j), us.at[j, i], ur.at[j, i], tensor=lax.rem(z + 1, nz))

    def down(i, j, first):
        src = own(i, j) if first else slot(down_buf, i, j)
        return remote(
            src, slot(down_buf, i, j), ds_.at[j, i], dr.at[j, i], tensor=lax.rem(z + nz - 1, nz)
        )

    def to_shard(j, a):
        peer = lax.rem(s + j, ns)
        n = grads[a].shape[0] // ns
        src = grads[a].at[pl.ds(pl.multiple_of(peer * n, n), n), :]
        return remote(src, shard_bufs[a].at[j - 1], ss.at[j - 1, a], sr.at[j - 1, a], shard=peer)

    for a in (3, 0, 1, 2):
        for j in range(1, ns):
            to_shard(j, a).start()

    for j in reversed(range(1, nz)):
        for i in range(len(parts)):

            @pl.when(z == 0)
            def _():
                up(i, j, True).start()

            @pl.when(z == nz - 1)
            def _():
                down(i, nz - 1 - j, True).start()

    def row_send(k):
        return remote(rowsum, row_buf.at[k - 1], rs.at[k - 1], rr.at[k - 1], tensor=lax.rem(z + k, nz))

    def vec_ctx(k, b):
        src, dst = ((vec, vec_c), (zvec, zvec_c))[b]
        return remote(src, dst.at[k - 1], vcs.at[k - 1, b], vcr.at[k - 1, b], ctx=lax.rem(c + k, nc))

    def vec_shard(j, b):
        src, dst = ((vec_own, vec_s), (zvec_own, zvec_s))[b]
        return remote(src, dst.at[j - 1], vss.at[j - 1, b], vsr.at[j - 1, b], shard=lax.rem(s + j, ns))

    def vec_z(k):
        return remote(out_zvec, zvec_z.at[k - 1], vzs.at[k - 1], vzr.at[k - 1], tensor=lax.rem(z + k, nz))

    for k in range(1, nz):
        row_send(k).start()
    for k in range(1, nc):
        for b in range(2):
            vec_ctx(k, b).start()

    row_back = remote(
        out_row.at[:, :, pl.ds(0, LANES)], row_halo, rhs, rhr, ctx=lax.rem(c + nc - 1, nc)
    )

    def rows_step():
        total = rowsum[...]
        for k in range(1, nz):
            row_send(k).wait_recv()
            total = total + row_buf[k - 1]
        out_row[...] = total

        @pl.when(c > 0)
        def _():
            row_back.start()

    def vec_step():
        for b in range(2):
            src, dst, slots = ((vec, vec_own, vec_c), (zvec, zvec_own, zvec_c))[b]
            total = src[...]
            for k in range(1, nc):
                vec_ctx(k, b).wait_recv()
                total = total + slots[k - 1]
            dst[...] = total
            for j in range(1, ns):
                vec_shard(j, b).start()

    def vec_next():
        for b in range(2):
            src, dst, slots = ((vec_own, out_vec, vec_s), (zvec_own, out_zvec, zvec_s))[b]
            total = src[...]
            for j in range(1, ns):
                vec_shard(j, b).wait_recv()
                total = total + slots[j - 1]
            dst[...] = total
        for k in range(1, nz):
            vec_z(k).start()

    def to_ctx(k, a):
        peer = lax.rem(c + k, nc)
        n = out_grads[a].shape[0]
        src = shard_bufs[a].at[0, pl.ds(pl.multiple_of(peer * n, n), n), :]
        return remote(src, ctx_bufs[a].at[k - 1], cs.at[k - 1, a], cr.at[k - 1, a], ctx=peer)

    def shard_step(a):
        n = out_grads[a].shape[0]
        for j in range(1, ns):
            to_shard(j, a).wait_recv()

        for k in list(range(1, nc)) + [0]:
            block = lax.rem(c + k, nc)
            there = pl.ds(pl.multiple_of(block * n, n), n)
            mine = pl.ds(pl.multiple_of((s * nc + block) * n, n), n)
            total = grads[a][mine, :].astype(F32)
            for j in range(1, ns):
                total = total + shard_bufs[a][j - 1, there, :].astype(F32)
            if k == 0:
                out_grads[a][...] = total
            else:
                shard_bufs[a][0, there, :] = total.astype(BF16)
                to_ctx(k, a).start()

    def ctx_step(a):
        for k in range(1, nc):
            to_ctx(k, a).wait_recv()
        total = out_grads[a][...]
        for k in range(1, nc):
            total = total + ctx_bufs[a][k - 1].astype(F32)
        out_grads[a][...] = total

    def line_step(j, i):
        q, r0, n = parts[i]
        t = nz - 1 - j

        @pl.when((z > 0) & (z < j))
        def _():
            up(i, j, False).wait_recv()
            up_buf[j, q, r0 : r0 + n, :] = (
                up_buf[j, q, r0 : r0 + n, :].astype(F32)
                + part[q, r0 : r0 + n, j * quarter : (j + 1) * quarter].astype(F32)
            ).astype(BF16)
            up(i, j, False).start()

        @pl.when((z < nz - 1) & (z > t))
        def _():
            down(i, t, False).wait_recv()
            down_buf[t, q, r0 : r0 + n, :] = (
                down_buf[t, q, r0 : r0 + n, :].astype(F32)
                + part[q, r0 : r0 + n, t * quarter : (t + 1) * quarter].astype(F32)
            ).astype(BF16)
            down(i, t, False).start()

    line = [
        functools.partial(line_step, j, i) for j in reversed(range(2, nz)) for i in range(len(parts))
    ]
    others = [functools.partial(shard_step, a) for a in (3, 0, 1, 2)] + [rows_step, vec_step, vec_next]
    for i in range(max(len(line), len(others))):
        if i < len(line):
            line[i]()
        if i < len(others):
            others[i]()
    ctx_step(3)
    mat_own[...] = out_grads[3][:, 0:mwidth].astype(BF16)

    def mat_send(k):
        return remote(
            mat_own, mat_buf.at[k - 1], ms.at[k - 1], mr.at[k - 1], tensor=lax.rem(z + k, nz)
        )

    for k in range(1, nz):
        mat_send(k).start()
    for a in range(3):
        ctx_step(a)
    for j in range(nz):
        for i in range(len(parts)):

            @pl.when((z == j) & (z > 0))
            def _():
                up(i, j, False).wait_recv()

            @pl.when((z == j) & (z < nz - 1))
            def _():
                down(i, j, False).wait_recv()

    mine = pl.ds(pl.multiple_of(z * quarter, quarter), quarter)
    out_part[...] = part[:, :, mine].astype(F32)

    @pl.when(z > 0)
    def _():
        out_part[...] += up_buf[z].astype(F32)

    @pl.when(z < nz - 1)
    def _():
        out_part[...] += down_buf[z].astype(F32)

    halo = remote(
        out_part.at[:, pl.ds(0, HALO), :], halo_buf, hs, hr, ctx=lax.rem(c + nc - 1, nc)
    )

    @pl.when(c > 0)
    def _():
        halo.start()

    total = out_grads[3][:, 0:mwidth]
    for k in range(1, nz):
        mat_send(k).wait_recv()
        total = total + mat_buf[k - 1].astype(F32)
    out_grads[3][:, 0:mwidth] = total
    vec_sum = out_zvec[...]
    for k in range(1, nz):
        vec_z(k).wait_recv()
        vec_sum = vec_sum + zvec_z[k - 1]
    for k in range(1, nz):
        vec_z(k).wait_send()
    out_zvec[...] = vec_sum

    @pl.when(c > 0)
    def _():
        row_back.wait_send()
        halo.wait_send()

    @pl.when(c < nc - 1)
    def _():
        row_back.wait_recv()
        tail = slice(rows - HALO, rows - HALO + LANES)
        out_row[:, :, tail] += row_halo[...]
        halo.wait_recv()
        out_part[:, rows - HALO :, :] += halo_buf[...]

    for j in reversed(range(1, nz)):
        for i in range(len(parts)):
            t = nz - 1 - j

            @pl.when(z < j)
            def _():
                up(i, j, False).wait_send()

            @pl.when(z > t)
            def _():
                down(i, t, False).wait_send()

    for a in range(4):
        for j in range(1, ns):
            to_shard(j, a).wait_send()
        for k in range(1, nc):
            to_ctx(k, a).wait_send()
    for k in range(1, nz):
        row_send(k).wait_send()
        mat_send(k).wait_send()
    for b in range(2):
        for k in range(1, nc):
            vec_ctx(k, b).wait_send()
        for j in range(1, ns):
            vec_shard(j, b).wait_send()


def reduce_all(part, rowsum, vec, zvec, grads, mwidth):
    ns, nc, nz = dims = sizes()
    seqs, rows, width = part.shape
    quarter = width // nz
    own = [(g.shape[0] // (ns * nc), g.shape[1]) for g in grads]
    dma = pltpu.SemaphoreType.DMA
    halves = 2 * seqs
    shape = jax.ShapeDtypeStruct
    buffers = [
        pltpu.VMEM((nz, seqs, rows, quarter), BF16),
        pltpu.VMEM((nz, seqs, rows, quarter), BF16),
        pltpu.VMEM((seqs, HALO, quarter), F32),
        pltpu.VMEM((nz - 1,) + rowsum.shape, F32),
        pltpu.VMEM(rowsum.shape[:2] + (LANES,), F32),
    ]
    buffers += [pltpu.VMEM((ns - 1, g.shape[0] // ns, g.shape[1]), BF16) for g in grads]
    buffers += [pltpu.VMEM((nc - 1,) + o, BF16) for o in own]
    block = own[3][0]
    buffers += [
        pltpu.VMEM((block, mwidth), BF16),
        pltpu.VMEM((nz - 1, block, mwidth), BF16),
        pltpu.VMEM((nc - 1,) + vec.shape, F32),
        pltpu.VMEM(vec.shape, F32),
        pltpu.VMEM((ns - 1,) + vec.shape, F32),
        pltpu.VMEM((nc - 1,) + zvec.shape, F32),
        pltpu.VMEM(zvec.shape, F32),
        pltpu.VMEM((ns - 1,) + zvec.shape, F32),
        pltpu.VMEM((nz - 1,) + zvec.shape, F32),
    ]
    semaphores = [dma((nz, halves))] * 4 + [dma] * 2 + [dma((nz - 1,))] * 2 + [dma] * 2
    semaphores += [dma((ns - 1, 4))] * 2 + [dma((nc - 1, 4))] * 2 + [dma((nz - 1,))] * 2
    semaphores += [dma((nc - 1, 2))] * 2 + [dma((ns - 1, 2))] * 2 + [dma((nz - 1,))] * 2
    return pl.pallas_call(
        functools.partial(reduce_kernel, dims, mwidth),
        out_shape=[
            shape((seqs, rows, quarter), F32),
            shape(rowsum.shape, F32),
            shape(vec.shape, F32),
            shape(zvec.shape, F32),
        ]
        + [shape(o, F32) for o in own],
        in_specs=[vmem_spec()] * 8,
        out_specs=[vmem_spec()] * 8,
        scratch_shapes=buffers + semaphores,
        compiler_params=pltpu.CompilerParams(
            collective_id=4, has_side_effects=True, vmem_limit_bytes=VMEM_ALL
        ),
        name="reduce_all",
    )(part, rowsum, vec, zvec, *grads)


def body(
    block_input,
    output_cotangent,
    norm_gain,
    gate_value_weight,
    matrix_weight,
    step_weight,
    out_weight,
    value_kernel,
    value_bias,
    matrix_kernel,
    matrix_bias,
    step_bias,
    decay_log,
    skip_gain,
    inner_gain,
):
    seqs, length, quarter = block_input.shape
    heads = step_bias.shape[0]
    inner = inner_gain.shape[0]
    head_width = inner // heads
    mwidth = matrix_weight.shape[1]
    block = matrix_weight.shape[0]
    ns, nc, nz = sizes()
    inner_total = inner * nz
    model_width = quarter * nz

    small_weight = jnp.concatenate(
        [
            matrix_weight,
            step_weight,
            norm_gain[:, None],
            jnp.zeros((block, LANES - heads - 1), BF16),
        ],
        axis=1,
    )
    X, GV, OW, SW = gather(
        block_input, gate_value_weight.reshape(block, 2 * inner), out_weight, small_weight
    )
    gain = SW[:, mwidth + heads].astype(F32).reshape(1, model_width)
    cot_late, X = lax.optimization_barrier((output_cotangent, X))
    full_cot = lax.all_gather(cot_late, "tensor", axis=2, tiled=True)

    lane_row = lambda array: jnp.pad(array, (0, LANES - heads))[None, :]
    rate_heads = -jnp.exp(decay_log)
    rate, sb = lane_row(rate_heads), lane_row(step_bias)
    skip = jnp.repeat(skip_gain, head_width)[None, :]
    ig = inner_gain[None, :]

    normed, gate_value, small, scale = project(X, gain, GV, SW)
    v, slope, y, starts, own, step, cum, carry, mat, mslope, end = forward(
        gate_value,
        small,
        value_kernel,
        value_bias[None, :],
        matrix_kernel,
        matrix_bias[None, :],
        sb,
        rate,
        heads,
    )
    states, ends = exchange(own, end, False)
    ssd, grad_inner, sums, start = gate_step(
        y, v, gate_value, full_cot, OW, cum, carry, mat, states, ends, ig, skip, heads
    )
    sums = token_sum(sums)
    gm, gz, normed_inner, part, adjoint, gvec = mixed_step(
        ssd, v, gate_value, grad_inner, sums, OW, cum, carry, mat, ig, skip, heads, inner_total, nz
    )
    share = lax.psum_scatter(part, "tensor", scatter_dimension=0, tiled=True)[0]
    block_output = (block_input.astype(F32) + share.astype(F32)).astype(BF16)
    adjoints, _ = exchange(adjoint, end, True)
    gx, gs, bvec, mvec, svec = backward(
        gm, v, slope, ssd, starts, carry, cum, step, mat, mslope, start, adjoints, ends,
        gate_value, small, value_kernel, matrix_kernel, sb, rate, skip, heads,
    )
    grad_part, rowsum, colsum = normed_grad(gz, gx, gs, normed, GV, SW)
    grads = (
        dot_tokens(normed, gz).astype(BF16),
        dot_tokens(normed, gx).astype(BF16),
        dot_tokens(full_cot, normed_inner).astype(BF16),
        dot_tokens(normed, gs).astype(BF16),
    )
    kernel_width = value_kernel.shape[0]
    tail = jnp.concatenate(
        [
            svec[0, :heads],
            rate_heads * svec[1, :heads],
            jnp.sum(gvec[1].reshape(heads, head_width), axis=1),
            jnp.zeros((inner - 3 * heads,), F32),
        ]
    )
    vec = jnp.concatenate(
        [
            bvec[: kernel_width + 1],
            gvec[0:1],
            tail[None, :],
            jnp.zeros((8 - kernel_width - 3, inner), F32),
        ],
        axis=0,
    )
    norm_part = colsum[0] / gain[0]
    flat = jnp.concatenate([mvec[: kernel_width + 1].reshape(-1), norm_part])
    zlanes = -(-flat.shape[0] // (8 * LANES)) * LANES
    zvec = jnp.pad(flat, (0, 8 * zlanes - flat.shape[0])).reshape(8, zlanes)

    grad_quarter, row_total, vec, zvec, gz_w, gx_w, ow_w, small_w = reduce_all(
        grad_part, rowsum, vec, zvec, grads, mwidth
    )
    z = lax.axis_index("tensor")
    feature = z * quarter
    gain_quarter = lax.dynamic_slice_in_dim(gain[0], feature, quarter, axis=0)
    scale_own = scale[:, HALO:, :1]
    normal = block_input.astype(F32) * scale_own
    row_mean = row_total[:, 0, HALO : HALO + length] / model_width
    input_grad = scale_own * (
        grad_quarter[:, HALO:] * gain_quarter - normal * row_mean[:, :, None]
    ) + output_cotangent.astype(F32)
    flat = zvec.reshape(-1)
    msize = (kernel_width + 1) * mwidth
    mgrads = flat[:msize].reshape(kernel_width + 1, mwidth)
    place = (lax.axis_index("shard") * nc + lax.axis_index("ctx")) * block
    norm_grad = lax.dynamic_slice_in_dim(flat[msize : msize + model_width], place, block, axis=0)
    tail = vec[kernel_width + 2]
    return (
        block_output,
        input_grad,
        norm_grad,
        jnp.stack([gz_w, gx_w], axis=1),
        small_w[:, :mwidth],
        small_w[:, mwidth : mwidth + heads],
        ow_w,
        vec[:kernel_width],
        vec[kernel_width],
        mgrads[:kernel_width],
        mgrads[kernel_width],
        tail[:heads],
        tail[heads : 2 * heads],
        tail[2 * heads : 3 * heads],
        vec[kernel_width + 1],
    )


def solution(mesh):
    placed = (
        P("shard", "ctx", "tensor"),
        P("shard", "ctx", "tensor"),
        P(("shard", "ctx")),
        P(("shard", "ctx"), None, "tensor"),
        P(("shard", "ctx"), None),
        P(("shard", "ctx"), "tensor"),
        P(("shard", "ctx"), "tensor"),
        P(None, "tensor"),
        P("tensor"),
        P(),
        P(),
        P("tensor"),
        P("tensor"),
        P("tensor"),
        P("tensor"),
    )
    return jax.shard_map(
        body,
        mesh=mesh,
        in_specs=placed,
        out_specs=(
            P("shard", "ctx", "tensor"),
            P("shard", "ctx", "tensor"),
            P(("shard", "ctx")),
            P(("shard", "ctx"), None, "tensor"),
            P(("shard", "ctx"), None),
            P(("shard", "ctx"), "tensor"),
            P(("shard", "ctx"), "tensor"),
            P(None, "tensor"),
            P("tensor"),
            P(),
            P(),
            P("tensor"),
            P("tensor"),
            P("tensor"),
            P("tensor"),
        ),
        check_vma=False,
    )
```
